32 devices in a mesh: replica: 8 (over z, core), group: 4 (over y, x).
Axes of the slice: x: 2, y: 2, z: 4, core: 2. Of those that a mesh axis runs over, the one named last changes fastest.
Arguments:
- deltas: bfloat16 [2, 8, 3072, 6144], P(None, 'replica', 'group'), may hold values from -8000 to 8000
- master: float32 [2, 3072, 6144], P(None, ('group', 'replica')), may hold values from -6 to 6
- momentum: float32 [2, 3072, 6144], P(None, ('group', 'replica')), may hold values from -6 to 6
Outputs:
- new_master: float32 [2, 3072, 6144], P(None, ('group', 'replica'))
- new_momentum: float32 [2, 3072, 6144], P(None, ('group', 'replica'))
- worker_params: bfloat16 [2, 3072, 6144], P(None, 'group')
The draws below stay inside these ranges and needn't reach their ends.
All inputs are finite; a program needn't handle non-finite values.
Results may differ from the reference program's by a relative error of at most 0.0065.
Values may be sent and summed in bfloat16 or wider, within the bound.
A program may use at most 128 MiB of HBM per device.

```python
import jax
import jax.numpy as jnp
from jax import lax

D = 6144
ROWS = 3072
FRAGS = 2
REPLICAS = 8


def draw_deltas(key, part):
    keys = jax.random.split(jax.random.fold_in(key, 17), 4)
    shape = (FRAGS, REPLICAS, ROWS, D)
    position = jnp.arange(ROWS, dtype=jnp.float32) / ROWS
    row_scale = jnp.exp(position * jnp.log(3.0)).reshape(1, 1, ROWS, 1)
    row_scale = row_scale * jnp.exp(jax.random.uniform(keys[0], (FRAGS, 1, ROWS, 1)) * jnp.log(10.0))
    col_scale = jnp.exp(jax.random.uniform(keys[1], (FRAGS, 1, 1, D)) * jnp.log(10.0))
    rep_scale = jnp.exp(jax.random.uniform(keys[2], (FRAGS, REPLICAS, 1, 1)) * jnp.log(3.0))
    values = jnp.clip(jax.random.normal(keys[3], shape), -4.0, 4.0)
    return (values * row_scale * col_scale * rep_scale).astype(jnp.bfloat16)


def steps_of(stream_key, dims, cuts, least, high):
    gain = 1.0
    for dim, blocks in cuts:
        draws = jax.random.uniform(jax.random.fold_in(jax.random.fold_in(stream_key, 6), dim), (blocks,), jnp.float32, least / len(cuts), high / len(cuts))
        gain = gain * jnp.repeat(jnp.exp(draws), dims[dim] // blocks).reshape((-1,) + (1,) * (len(dims) - 1 - dim))
    return gain


def centred(key, dims, width, most, pieces=(), kind=jnp.bfloat16):
    loudness = steps_of(key, dims, pieces, -0.22, 0.18) if pieces else 1.0
    entries = jax.random.normal(key, dims, jnp.float32) * width * loudness
    return jnp.minimum(jnp.maximum(entries, -most), most).astype(kind)


def setup_inputs(seed: int = 0) -> dict:
    key_of = jax.random.split(jax.random.key(seed), 4)
    deltas = draw_deltas(jax.random.fold_in(key_of[3], 71), 0)
    master = centred(key_of[1], (FRAGS, ROWS, D), 1.0, 6.0, ((1, 32),), jnp.float32)
    momentum = centred(key_of[2], (FRAGS, ROWS, D), 0.5, 6.0, ((1, 32),), jnp.float32)
    return {"deltas": deltas, "master": master, "momentum": momentum}


def reference(deltas, master, momentum):

    def add_one(index, total):
        piece = lax.dynamic_index_in_dim(deltas, index, 1, keepdims=False)
        return total + piece.astype(jnp.float32)
    start = jnp.zeros((FRAGS, ROWS, D), jnp.float32)
    averaged = lax.fori_loop(0, REPLICAS, add_one, start) / REPLICAS
    squares = lax.optimization_barrier(jnp.sum(averaged * averaged, axis=(1, 2), keepdims=True))
    factor = jnp.minimum(1.0, 0.25 * jnp.sqrt(float(ROWS * D)) / (jnp.sqrt(squares) + 1e-06))
    clipped = factor * averaged
    new_momentum = 0.9 * momentum + clipped
    new_master = master - 0.7 * (clipped + 0.9 * new_momentum)
    return (new_master, new_momentum, new_master.astype(jnp.bfloat16))
```

```python
import functools

import jax
import jax.numpy as jnp
from jax import lax
from jax.experimental import pallas as pl
from jax.experimental.pallas import tpu as pltpu
from jax.sharding import PartitionSpec as P

MESH = pl.DeviceIdType.MESH
CORES = 2


def sync_kernel(
    n, groups, width,
    deltas, master, momentum,
    out_master, out_momentum, out_params,
    mine, theirs, arrived, average, mas, mom, params, sq_rows, sq_groups, sq_send,
    load_sem, pair_send, pair_recv, line_send, line_recv,
    right_send, left_send, twin_send, ag_recv, twin_recv,
    keep_sem, state_in, state_out, sq_send_a, sq_recv_a, sq_send_b, sq_recv_b,
):
    frags, m, pieces, rc, depth = mine.shape
    me = lax.axis_index("replica")
    grp = lax.axis_index("group")
    z, c = me // CORES, me % CORES
    twin = z * CORES + (1 - c)
    count = float(n * groups * pieces * rc * depth)

    barrier = pltpu.get_barrier_semaphore()
    for d in range(1, n):
        pl.semaphore_signal(barrier, inc=1, device_id=(lax.rem(me + d, n), grp), device_id_type=MESH)
    for d in range(1, groups):
        pl.semaphore_signal(barrier, inc=1, device_id=(me, lax.rem(grp + d, groups)), device_id_type=MESH)
    pl.semaphore_wait(barrier, n + groups - 2)

    def remote(src, dst, send, recv, replica, group=grp):
        return pltpu.make_async_remote_copy(
            src_ref=src, dst_ref=dst, send_sem=send, recv_sem=recv,
            device_id=(replica, group), device_id_type=MESH,
        )

    def load(f, o, k):
        return pltpu.make_async_copy(deltas.at[f, o * CORES + c, k], mine.at[f, o, k], load_sem.at[f, o, k])

    def pair(f, o, k):
        return remote(
            deltas.at[f, o * CORES + (1 - c), k], theirs.at[f, o, k],
            pair_send.at[f, o, k], pair_recv.at[f, o, k], twin,
        )

    def line(f, o, k, slot, to):
        return remote(
            mine.at[f, o, k], arrived.at[f, slot, k], line_send.at[f, o, k], line_recv.at[f, slot, k], to
        )

    def each_piece(body):
        def step(k, carry):
            body(k)
            return carry
        lax.fori_loop(0, pieces, step, 0)

    def each_column(body, init=0):
        def step(j, carry):
            return body(pl.ds(pl.multiple_of(j * width, width), width), carry)
        return lax.fori_loop(0, depth // width, step, init)

    def state(f):
        return (
            pltpu.make_async_copy(master.at[f], mas.at[f], state_in.at[0, f]),
            pltpu.make_async_copy(momentum.at[f], mom.at[f], state_in.at[1, f]),
        )

    def state_back(f):
        return (
            pltpu.make_async_copy(mas.at[f], out_master.at[f], state_out.at[0, f]),
            pltpu.make_async_copy(mom.at[f], out_momentum.at[f], state_out.at[1, f]),
        )

    def by_distance(s, body):
        @pl.when(z + s < m)
        def _():
            body(z + s, 1)

        if s > 0:
            @pl.when(z - s >= 0)
            def _():
                body(z - s, -1)

    def fetch(f):
        for s in range(m - 1, -1, -1):
            def go(k):
                def one(o, way):
                    load(f, o, k).start()
                    pair(f, o, k).start()
                by_distance(s, one)
            each_piece(go)
        for copy in state(f):
            copy.start()

    def add_pair(f, o, k, cols):
        return mine[f, o, k, :, cols].astype(jnp.float32) + theirs[f, o, k, :, cols].astype(jnp.float32)

    def reduce_far(f, s):
        def go(k):
            def one(o, way):
                load(f, o, k).wait()
                pair(f, o, k).wait_recv()
                to = me + way * CORES
                back = z - way
                inner = (back >= 0) & (back < m)

                @pl.when(inner)
                def _():
                    line(f, o, k, o, to).wait_recv()

                    def body(cols, carry):
                        total = add_pair(f, o, k, cols) + arrived[f, o, k, :, cols].astype(jnp.float32)
                        mine[f, o, k, :, cols] = total.astype(jnp.bfloat16)
                        return carry
                    each_column(body)

                @pl.when(jnp.logical_not(inner))
                def _():
                    def body(cols, carry):
                        mine[f, o, k, :, cols] = add_pair(f, o, k, cols).astype(jnp.bfloat16)
                        return carry
                    each_column(body)

                if s == 1 and way == -1:
                    line(f, o, k, m, to).start()
                else:
                    line(f, o, k, o, to).start()
            by_distance(s, one)
        each_piece(go)

    def reduce_own(f):
        def go(k):
            load(f, z, k).wait()
            pair(f, z, k).wait_recv()

            def start(cols, carry):
                average[f, k, :, cols] = add_pair(f, z, k, cols)
                return carry
            each_column(start)

            for slot, there in ((z, z > 0), (m, z < m - 1)):
                @pl.when(there)
                def _(slot=slot):
                    line(f, z, k, slot, twin).wait_recv()

                    def body(cols, carry):
                        average[f, k, :, cols] += arrived[f, slot, k, :, cols].astype(jnp.float32)
                        return carry
                    each_column(body)
        each_piece(go)

        def piece_squares(k, total):
            def body(cols, total):
                value = average[f, k, :, cols] * (1.0 / n)
                average[f, k, :, cols] = value
                square = value * value
                for r in range(0, rc, 8):
                    for q in range(0, width, 128):
                        total = total + square[r:r + 8, q:q + 128]
                return total
            return each_column(body, total)
        total = lax.fori_loop(0, pieces, piece_squares, jnp.zeros((8, 128), jnp.float32))
        sq_send[f, 0] = total
        sq_rows[f, me] = total
        for d in range(1, n):
            squares_a(f, me, lax.rem(me + d, n), d).start()

    def squares_a(f, slot, to, d):
        return remote(sq_send.at[f, 0], sq_rows.at[f, slot], sq_send_a.at[f, d], sq_recv_a.at[f, slot], to)

    def squares_b(f, slot, to, d):
        return remote(sq_send.at[f, 1], sq_groups.at[f, slot], sq_send_b.at[f, d], sq_recv_b.at[f, slot], me, to)

    def factor_of(f):
        for d in range(1, n):
            squares_a(f, lax.rem(me + d, n), lax.rem(me + d, n), d).wait_recv()
        total = sq_rows[f, 0]
        for r in range(1, n):
            total = total + sq_rows[f, r]
        sq_send[f, 1] = total
        sq_groups[f, grp] = total
        for d in range(1, groups):
            squares_b(f, grp, lax.rem(grp + d, groups), d).start()
        for d in range(1, groups):
            squares_b(f, lax.rem(grp + d, groups), lax.rem(grp + d, groups), d).wait_recv()
        total = sq_groups[f, 0]
        for r in range(1, groups):
            total = total + sq_groups[f, r]
        squares = jnp.sum(jnp.sum(total, axis=1, keepdims=True), axis=0, keepdims=True)
        bound = 0.25 * count ** 0.5
        return jnp.minimum(1.0, bound / (jnp.sqrt(squares) + 1e-06))

    def keep(f, k):
        return pltpu.make_async_copy(params.at[f, k], out_params.at[f, me, k], keep_sem.at[f, k])

    def place(f, o, k):
        return out_params.at[f, o * CORES + c, k]

    def send_right(f, o, k, src):
        return remote(src, place(f, o, k), right_send.at[f, o, k], ag_recv.at[f, o, k], me + CORES)

    def send_left(f, o, k, src):
        return remote(src, place(f, o, k), left_send.at[f, o, k], ag_recv.at[f, o, k], me - CORES)

    def send_twin(f, o, k, src):
        return remote(src, place(f, o, k), twin_send.at[f, o, k], twin_recv.at[f, o, k], twin)

    def update(f):
        factor = factor_of(f)
        for copy in state(f):
            copy.wait()

        def go(k):
            def body(cols, carry):
                clipped = factor * average[f, k, :, cols]
                moved = 0.9 * mom[f, k, :, cols] + clipped
                updated = mas[f, k, :, cols] - 0.7 * (clipped + 0.9 * moved)
                mom[f, k, :, cols] = moved
                mas[f, k, :, cols] = updated
                params[f, k, :, cols] = updated.astype(jnp.bfloat16)
                return carry
            each_column(body)

            @pl.when(z < m - 1)
            def _():
                send_right(f, z, k, params.at[f, k]).start()

            @pl.when(z > 0)
            def _():
                send_left(f, z, k, params.at[f, k]).start()
            send_twin(f, z, k, params.at[f, k]).start()
            keep(f, k).start()
        each_piece(go)
        for copy in state_back(f):
            copy.start()

    def spread(f, s):
        def go(k):
            def one(o, way):
                src = place(f, o, k)
                send_right(f, o, k, src).wait_recv()
                if way == 1:
                    @pl.when(z > 0)
                    def _():
                        send_left(f, o, k, src).start()
                else:
                    @pl.when(z < m - 1)
                    def _():
                        send_right(f, o, k, src).start()
                send_twin(f, o, k, src).start()
            by_distance(s, one)
        each_piece(go)

    def finish(f):
        def go(k):
            def every(o, carry):
                pair(f, o, k).wait_send()
                src = place(f, o, k)
                send_twin(f, o, k, src).wait_send()
                remote(
                    src, out_params.at[f, o * CORES + (1 - c), k],
                    twin_send.at[f, o, k], twin_recv.at[f, o, k], twin,
                ).wait_recv()

                @pl.when(o != z)
                def _():
                    line(f, o, k, o, twin).wait_send()

                @pl.when((z < m - 1) & (o <= z))
                def _():
                    send_right(f, o, k, src).wait_send()

                @pl.when((z > 0) & (o >= z))
                def _():
                    send_left(f, o, k, src).wait_send()
                return carry
            lax.fori_loop(0, m, every, 0)
            keep(f, k).wait()
        each_piece(go)
        for d in range(1, n):
            squares_a(f, me, twin, d).wait_send()
        for d in range(1, groups):
            squares_b(f, grp, lax.rem(grp + d, groups), d).wait_send()
        for copy in state_back(f):
            copy.wait()

    for f in range(frags):
        fetch(f)
    for s in range(m - 1, 0, -1):
        reduce_far(0, s)
    reduce_own(0)
    for f in range(frags):
        if f + 1 < frags:
            reduce_far(f + 1, m - 1)
        update(f)
        for s in range(1, m):
            if f + 1 < frags and m - 1 - s > 0:
                reduce_far(f + 1, m - 1 - s)
            if f + 1 < frags and s == m - 1:
                reduce_own(f + 1)
            spread(f, s)
    for f in range(frags):
        finish(f)


def on_device(deltas, master, momentum):
    n, groups = lax.axis_size("replica"), lax.axis_size("group")
    frags, rows, depth = master.shape
    m = n // CORES
    pieces = 3 if rows % 24 == 0 else 1
    rc = rows // pieces
    width = 512 if depth % 512 == 0 else 128
    state = (frags, pieces, rc, depth)
    dma = pltpu.SemaphoreType.DMA
    per_block = dma((frags, m, pieces))
    hbm = pl.BlockSpec(memory_space=pl.ANY)
    new_master, new_momentum, params = pl.pallas_call(
        functools.partial(sync_kernel, n, groups, width),
        out_shape=(
            jax.ShapeDtypeStruct(state, jnp.float32),
            jax.ShapeDtypeStruct(state, jnp.float32),
            jax.ShapeDtypeStruct((frags, n, pieces, rc, depth), jnp.bfloat16),
        ),
        in_specs=[hbm] * 3,
        out_specs=(hbm,) * 3,
        scratch_shapes=[
            pltpu.VMEM((frags, m, pieces, rc, depth), jnp.bfloat16),
            pltpu.VMEM((frags, m, pieces, rc, depth), jnp.bfloat16),
            pltpu.VMEM((frags, m + 1, pieces, rc, depth), jnp.bfloat16),
            pltpu.VMEM(state, jnp.float32),
            pltpu.VMEM(state, jnp.float32),
            pltpu.VMEM(state, jnp.float32),
            pltpu.VMEM(state, jnp.bfloat16),
            pltpu.VMEM((frags, n, 8, 128), jnp.float32),
            pltpu.VMEM((frags, groups, 8, 128), jnp.float32),
            pltpu.VMEM((frags, 2, 8, 128), jnp.float32),
            per_block, per_block, per_block, per_block, dma((frags, m + 1, pieces)),
            per_block, per_block, per_block, per_block, per_block,
            dma((frags, pieces)), dma((2, frags)), dma((2, frags)),
            dma((frags, n)), dma((frags, n)), dma((frags, groups)), dma((frags, groups)),
        ],
        compiler_params=pltpu.CompilerParams(
            collective_id=0, has_side_effects=True, vmem_limit_bytes=62 * 1024 * 1024
        ),
    )(
        deltas.reshape(frags, n, pieces, rc, depth),
        master.reshape(state),
        momentum.reshape(state),
    )
    return (
        new_master.reshape(master.shape),
        new_momentum.reshape(master.shape),
        params.reshape(frags, n * rows, depth),
    )


def solution(mesh):
    return jax.shard_map(
        on_device,
        mesh=mesh,
        in_specs=(
            P(None, "replica", "group", None),
            P(None, ("group", "replica"), None),
            P(None, ("group", "replica"), None),
        ),
        out_specs=(
            P(None, ("group", "replica"), None),
            P(None, ("group", "replica"), None),
            P(None, "group", None),
        ),
        check_vma=False,
    )
```
